32 devices in a mesh: mem: 4 (over x, core), slab: 8 (over z, y).
Axes of the slice: x: 2, y: 2, z: 4, core: 2. Of those that a mesh axis runs over, the one named last changes fastest.
Arguments:
- anomalies: bfloat16 [8, 4096, 4096], P('mem', 'slab'), may hold values from -2.390625 to 2.390625
- increment: float32 [4096, 4096], P('slab'), may hold values from -6 to 6
- spectrum: float32 [4096, 4096], P(None, 'slab'), may hold values from 0.01 to 2, as said below
Outputs:
- product: float32 [4096, 4096], P('slab')
The draws below stay inside these ranges and needn't reach their ends.
Inputs may be any that keep to these rules, and one draw needn't show every extreme that they name: spectrum[k, l] equals spectrum[(4096 - k) % 4096, (4096 - l) % 4096], and is positive.
All inputs are finite; a program needn't handle non-finite values.
Results may differ from the reference program's by a relative error of at most 0.0003.
Values sent between devices are 32-bit elements; how exact they have to be, the bound alone decides.
A program may use at most 192 MiB of HBM per device.

```python
import jax
import jax.numpy as jnp
from jax import lax

NX = 4096
NY = 4096
MEMBERS = 8


def draw_spectrum(key, part):
    logs = jax.random.uniform(key, (NX, NY), jnp.float32, jnp.log(0.05), 0.0)
    values = jnp.exp(logs)
    mirrored = jnp.roll(jnp.flip(values, (0, 1)), 1, (0, 1))
    result = 0.5 * (values + mirrored)
    return result


def shard_levels(own_key, extent, split, low, top_value):
    loudness, own = 1.0, jax.random.fold_in(own_key, 6)
    for dim, shards_of in split:
        steps = jnp.exp(jax.random.uniform(jax.random.fold_in(own, dim), (shards_of,), jnp.float32, low / len(split), top_value / len(split)))
        loudness = loudness * jnp.repeat(steps, extent[dim] // shards_of).reshape([-1 if axis == dim else 1 for axis in range(len(extent))])
    return loudness


def noise(key, shape, spread, limit, pieces=(), held_as=jnp.bfloat16):
    level = shard_levels(key, shape, pieces, -0.22, 0.18) if pieces else 1.0
    array = jax.random.normal(key, shape, jnp.float32) * spread * level
    return jnp.minimum(jnp.maximum(array, -limit), limit).astype(held_as)


def setup_inputs(seed: int = 0) -> dict:
    streams_of = jax.random.split(jax.random.key(seed), 4)
    anomalies = noise(streams_of[0], (MEMBERS, NX, NY), 0.4, 2.390625, ((0, 4), (1, 8)))
    increment = noise(streams_of[1], (NX, NY), 1.0, 6.0, ((0, 8),), jnp.float32)
    spectrum = draw_spectrum(jax.random.fold_in(streams_of[3], 71), 0)
    return {"anomalies": anomalies, "increment": increment, "spectrum": spectrum}


def reference(anomalies, increment, spectrum):
    def member_term(index, total):
        member = lax.dynamic_index_in_dim(anomalies, index, 0, keepdims=False).astype(jnp.float32)
        field = member * increment
        waves = jnp.fft.fft2(field)
        filtered = jnp.real(jnp.fft.ifft2(waves * spectrum))
        return total + member * filtered

    start = jnp.zeros((NX, NY), jnp.float32)
    return lax.fori_loop(0, MEMBERS, member_term, start)
```

```python
import functools
import math

import jax
import jax.numpy as jnp
import numpy as np
from jax import lax
from jax.experimental import pallas as pl
from jax.experimental.pallas import tpu as pltpu
from jax.sharding import PartitionSpec as P

LANES = 128


def butterflies(parts, sign):
    n = len(parts)
    if n == 1:
        return parts
    even = butterflies(parts[0::2], sign)
    odd = butterflies(parts[1::2], sign)
    low, high = [], []
    for k in range(n // 2):
        (er, ei), (pr, pi) = even[k], odd[k]
        if k == 0:
            tr, ti = pr, pi
        elif 4 * k == n:
            tr, ti = (pi, -pr) if sign < 0 else (-pi, pr)
        elif 8 * k == n:
            h = math.sqrt(0.5)
            tr, ti = ((pr + pi) * h, (pi - pr) * h) if sign < 0 else ((pr - pi) * h, (pr + pi) * h)
        elif 8 * k == 3 * n:
            h = math.sqrt(0.5)
            tr, ti = ((pi - pr) * h, -(pr + pi) * h) if sign < 0 else (-(pr + pi) * h, (pr - pi) * h)
        else:
            angle = sign * 2.0 * math.pi * k / n
            c, s = math.cos(angle), math.sin(angle)
            tr, ti = pr * c - pi * s, pr * s + pi * c
        low.append((er + tr, ei + ti))
        high.append((er - tr, ei - ti))
    return low + high


def split(x):
    hi = x.astype(jnp.bfloat16)
    return hi, (x - hi.astype(jnp.float32)).astype(jnp.bfloat16)


def dot(a, b):
    return jnp.dot(a, b, preferred_element_type=jnp.float32)


def lane_block(sign):
    idx = np.arange(LANES)
    angle = sign * 2.0 * np.pi / LANES * (idx[:, None] * idx[None, :] % LANES)
    c, s = np.cos(angle), np.sin(angle)
    return np.block([[c, s], [-s, c]])


def split_table(table):
    hi_np = np.asarray(table.astype(jnp.bfloat16), np.float64)
    return np.stack([table.astype(jnp.bfloat16), (table - hi_np).astype(jnp.bfloat16)])


def twist(first):
    a, b = np.arange(first), np.arange(LANES)
    angle = -2.0 * np.pi / (first * LANES) * (a[:, None] * b[None, :])
    return np.stack([np.cos(angle), np.sin(angle)]).astype(np.float32)


def turned_twist(first, slabs):
    a, b, own = np.arange(first), np.arange(LANES), np.arange(slabs)
    step = first * LANES // slabs
    turns = a[None, :, None] * b + own[:, None, None] * step * b
    angle = -2.0 * np.pi / (first * LANES) * (turns % (first * LANES))
    return np.stack([np.cos(angle), np.sin(angle)], axis=1).astype(np.float32)


def exchange(tiles, group):
    lane = lax.broadcasted_iota(jnp.int32, tiles[0].shape, 1)
    step = 1
    while step * group < LANES:
        width = step * group
        upper = (lane & width) != 0
        out = list(tiles)
        for t in range(len(tiles)):
            if not t & step:
                a, b = tiles[t], tiles[t + step]
                out[t] = jnp.where(upper, pltpu.roll(b, width, 1), a)
                out[t + step] = jnp.where(upper, b, pltpu.roll(a, LANES - width, 1))
        tiles = out
        step *= 2
    return tiles


def lane_matmul(y, w_ref, rows, count):
    @pl.loop(0, count)
    def _(i):
        at = pl.ds(pl.multiple_of(i * rows, rows), rows)
        hi, lo = split(y[at, :])
        y[at, :] = dot(hi, w_ref[0]) + (dot(lo, w_ref[0]) + dot(hi, w_ref[1]))


def rows_forward(first, slabs, pieces, anom, incr, w_ref, tw, *rest):
    outs, (f, y) = rest[:-2], rest[-2:]
    block = incr.shape[0]
    group = LANES // slabs
    per_out = first // slabs // pieces

    @pl.loop(0, block // 16)
    def _(g):
        at = pl.ds(pl.multiple_of(g * 16, 16), 16)
        inc = incr[at, :]
        f[0, at, :] = anom[0, at, :].astype(jnp.float32) * inc
        f[1, at, :] = anom[1, at, :].astype(jnp.float32) * inc

    @pl.loop(0, block // 8)
    def _(g):
        at = pl.ds(pl.multiple_of(g * 8, 8), 8)
        parts = [
            (f[0, at, a * LANES:(a + 1) * LANES], f[1, at, a * LANES:(a + 1) * LANES])
            for a in range(first)
        ]
        for c, (r, i) in enumerate(butterflies(parts, -1.0)):
            tr, ti = tw[0, c:c + 1, :], tw[1, c:c + 1, :]
            to = pl.ds(pl.multiple_of(c * block + g * 8, 8), 8)
            y[to, :LANES] = r * tr - i * ti
            y[to, LANES:] = r * ti + i * tr

    lane_matmul(y, w_ref, 4 * block, first // 4)

    @pl.loop(0, block // 8)
    def _(g):
        at = pl.ds(pl.multiple_of(g * 8, 8), 8)
        for q in range(first // slabs):
            base = q % per_out * 2 * LANES
            for half in range(2):
                lanes = slice(half * LANES, (half + 1) * LANES)
                tiles = [
                    y[pl.ds(pl.multiple_of((q * slabs + c) * block + g * 8, 8), 8), lanes]
                    for c in range(slabs)
                ]
                for s, tile in enumerate(exchange(tiles, group)):
                    to = slice(base + half * LANES, base + (half + 1) * LANES)
                    outs[q // per_out * slabs + s][at, to] = tile


def rows_inverse(first, slabs, core, anom, w_ref, tw, *rest):
    ins, (mine, give), (f, y) = rest[:-4], rest[-4:-2], rest[-2:]
    block = mine.shape[0]
    group = LANES // slabs

    @pl.loop(0, block // 8)
    def _(g):
        at = pl.ds(pl.multiple_of(g * 8, 8), 8)
        for q in range(first // slabs):
            for half in range(2):
                lanes = slice(half * LANES, (half + 1) * LANES)
                tiles = [ins[q * slabs + -s % slabs][at, lanes] for s in range(slabs)]
                for c, tile in enumerate(exchange(tiles, group)):
                    to = pl.ds(pl.multiple_of((q * slabs + c) * block + g * 8, 8), 8)
                    y[to, lanes] = tile

    lane_matmul(y, w_ref, 4 * block, first // 4)

    @pl.loop(0, block // 8)
    def _(g):
        at = pl.ds(pl.multiple_of(g * 8, 8), 8)
        parts = []
        for c in range(first):
            src = pl.ds(pl.multiple_of(c * block + g * 8, 8), 8)
            r, i = y[src, :LANES], y[src, LANES:]
            tr, ti = tw[0, c:c + 1, :], tw[1, c:c + 1, :]
            parts.append((r * tr + i * ti, i * tr - r * ti))
        for a, (r, i) in enumerate(butterflies(parts, 1.0)):
            f[0, at, a * LANES:(a + 1) * LANES] = r
            f[1, at, a * LANES:(a + 1) * LANES] = i

    def write(out):
        @pl.loop(0, block // 16)
        def _(g):
            at = pl.ds(pl.multiple_of(g * 16, 16), 16)
            out[at, :] = anom[0, at, :].astype(jnp.float32) * f[0, at, :] + anom[1, at, :].astype(
                jnp.float32
            ) * f[1, at, :]

    pl.when(pl.program_id(0) == 0)(lambda: write(mine))
    pl.when(pl.program_id(0) == 1)(lambda: write(give))


def columns(first, slabs, heights, offsets, bands, spec, w_f, w_i, tw, *rest):
    count, (x, y, o, in_sems, out_sems) = len(heights) * slabs, rest[-5:]
    ins, outs = rest[:count], rest[count:-5]
    rows = x.shape[1]
    me = lax.axis_index("slab")

    def arrival(k):
        part, j = divmod(k, slabs)
        at = pl.ds(sum(heights[:part]), heights[part])
        source = ins[k].at[:, pl.ds(offsets[part], 2 * LANES)]
        return pltpu.make_async_copy(source, x.at[(me + slabs - j) % slabs, at, :], in_sems.at[k])

    def departure(k):
        part, j = divmod(k, slabs)
        at = pl.ds(sum(bands[:part]), bands[part])
        return pltpu.make_async_copy(o.at[(me + j) % slabs, at, :], outs[k], out_sems.at[k])

    for k in range(count):
        arrival(k).start()
    for k in range(count):
        arrival(k).wait()

    @pl.loop(0, LANES // 8)
    def _(g):
        parts = []
        for a in range(first):
            s, r = divmod(a * LANES, rows)
            at = pl.ds(pl.multiple_of(r + g * 8, 8), 8)
            parts.append((x[s, at, :LANES], x[s, at, LANES:]))
        for c, (r, i) in enumerate(butterflies(parts, -1.0)):
            at = pl.ds(pl.multiple_of(g * 8, 8), 8)
            im = pl.ds(pl.multiple_of(LANES + g * 8, 8), 8)
            tr, ti = tw[0, c, at, :], tw[1, c, at, :]
            lanes = slice(c % 2 * LANES, (c % 2 + 1) * LANES)
            y[c // 2, at, lanes] = r * tr - i * ti
            y[c // 2, im, lanes] = r * ti + i * tr

    @pl.loop(0, first // 2)
    def _(p):
        hi, lo = split(y[p])
        z = dot(w_f[0], hi) + (dot(w_f[0], lo) + dot(w_f[1], hi))
        m = jnp.concatenate([spec[2 * p], spec[2 * p + 1]], axis=1)
        hi, lo = split(z * jnp.concatenate([m, m], axis=0))
        y[p] = dot(w_i[0], hi) + (dot(w_i[0], lo) + dot(w_i[1], hi))

    @pl.loop(0, LANES // 8)
    def _(g):
        at = pl.ds(pl.multiple_of(g * 8, 8), 8)
        im = pl.ds(pl.multiple_of(LANES + g * 8, 8), 8)
        parts = []
        for c in range(first):
            lanes = slice(c % 2 * LANES, (c % 2 + 1) * LANES)
            r, i = y[c // 2, at, lanes], y[c // 2, im, lanes]
            tr, ti = tw[0, c, at, :], tw[1, c, at, :]
            parts.append((r * tr + i * ti, i * tr - r * ti))
        for a, (r, i) in enumerate(butterflies(parts, 1.0)):
            s, row = divmod(a * LANES, rows)
            to = pl.ds(pl.multiple_of(row + g * 8, 8), 8)
            o[s, to, :LANES] = r
            o[s, to, LANES:] = i

    for k in range(len(bands) * slabs):
        departure(k).start()
    for k in range(len(bands) * slabs):
        departure(k).wait()


def place(core, a, b, *rest):
    out = rest[-1]

    @pl.when(pl.program_id(0) == 0)
    def _():
        out[...] = a[...]

    @pl.when(pl.program_id(0) == 1)
    def _():
        out[...] = b[...]


def per_device(slabs, groups, anomalies, increment, spectrum):
    f32 = jnp.float32
    members, rows, cols = anomalies.shape
    total_rows, own = spectrum.shape
    first, first_x = cols // LANES, total_rows // LANES
    pieces = first // slabs
    block = min(64, rows // 2)
    heights = (block, rows - block)
    bands = (2 * block,) * (rows // block // 2 - 1) + (block, block)
    width = 2 * LANES
    vmem = 67043328
    w_f, w_i = split_table(lane_block(-1.0)), split_table(lane_block(1.0))
    w_ft = split_table(lane_block(-1.0).T)
    w_it = split_table(lane_block(1.0).T)
    me, core = lax.axis_index("slab"), lax.axis_index("mem") % 2
    core = core.reshape(1)
    tw = lax.dynamic_index_in_dim(jnp.asarray(turned_twist(first, slabs)), me, 0, False)
    tw_x = jnp.broadcast_to(jnp.asarray(twist(first_x))[..., None], (2, first_x, LANES, LANES))
    group = LANES // slabs

    order = np.arange(own).reshape(group, pieces, slabs).transpose(1, 2, 0).reshape(-1)
    pick = np.zeros((own, own), np.float32)
    pick[order, np.arange(own)] = 1.0 / (total_rows * cols)
    spec = jnp.dot(spectrum, pick, precision=lax.Precision.HIGHEST)
    spec = spec.reshape(LANES, first_x, own).transpose(1, 0, 2)

    whole = lambda a: pl.BlockSpec(a.shape, lambda *_: (0,) * a.ndim)
    params = lambda: pltpu.CompilerParams(vmem_limit_bytes=vmem)
    cost = lambda n: pl.CostEstimate(flops=n * 3000, bytes_accessed=n * 16, transcendentals=0)
    shape = lambda *dims: jax.ShapeDtypeStruct(dims, f32)
    anywhere = pl.BlockSpec(memory_space=pltpu.HBM)

    def scratch(n):
        return [pltpu.VMEM((2, n, cols), f32), pltpu.VMEM((first * n, 2 * LANES), f32)]

    def sent(arrays):
        rings = [[(s, (s + j) % slabs) for s in range(slabs)] for j in range(slabs)]
        return [a if j == 0 else lax.ppermute(a, "slab", rings[j]) for j, a in enumerate(arrays)]

    def forward(start, n, split):
        across = width * pieces // split
        return pl.pallas_call(
            functools.partial(rows_forward, first, slabs, split),
            grid=(n // block,),
            in_specs=[
                pl.BlockSpec((2, block, cols), lambda i: (0, start // block + i, 0)),
                pl.BlockSpec((block, cols), lambda i: (start // block + i, 0)),
                whole(w_f),
                whole(tw),
            ],
            out_specs=[pl.BlockSpec((block, across), lambda i: (i, 0))] * (split * slabs),
            out_shape=[shape(n, across)] * (split * slabs),
            scratch_shapes=scratch(block),
            compiler_params=params(),
            cost_estimate=cost(n * cols),
        )(anomalies, increment, w_f, tw)

    opening = sent(forward(0, heights[0], 1))
    waves = forward(heights[0], heights[1], pieces)
    arrived = [sent(waves[p * slabs:(p + 1) * slabs]) for p in range(pieces)]

    back = []
    for p in range(pieces):
        cuts = bands if p == pieces - 1 else (rows,)
        filtered = pl.pallas_call(
            functools.partial(columns, first_x, slabs, heights, (p * width, 0), cuts),
            grid=(1,),
            in_specs=[
                pl.BlockSpec((first_x, LANES, LANES), lambda i, p=p: (0, 0, p)),
                whole(w_ft),
                whole(w_it),
                whole(tw_x),
            ]
            + [anywhere] * (2 * slabs),
            out_specs=[anywhere] * (len(cuts) * slabs),
            out_shape=[shape(n, width) for n in cuts for _ in range(slabs)],
            scratch_shapes=[
                pltpu.VMEM((slabs, rows, width), f32),
                pltpu.VMEM((first_x // 2, 2 * LANES, 2 * LANES), f32),
                pltpu.VMEM((slabs, rows, width), f32),
                pltpu.SemaphoreType.DMA((2 * slabs,)),
                pltpu.SemaphoreType.DMA((len(cuts) * slabs,)),
            ],
            compiler_params=params(),
            cost_estimate=cost(total_rows * width),
        )(spec, w_ft, w_it, tw_x, *opening, *arrived[p])
        back.append([sent(filtered[h * slabs:(h + 1) * slabs]) for h in range(len(cuts))])

    swap = lambda a, bit: lax.ppermute(a, "mem", [(m, m ^ bit) for m in range(groups)])
    product = None
    for h, n in enumerate(bands):
        half = n // 2
        at = sum(bands[:h]) // half
        here = lambda i, c, at=at: (at + (i + c[0]) % 2, 0)
        local = lambda i, c: ((i + c[0]) % 2, 0)
        kept = lambda i, c: (0, 0)
        whole_of = lambda a: pl.BlockSpec(a.shape, lambda *_, nd=a.ndim: (0,) * nd)
        ins, specs = [], []
        for p in range(pieces):
            last = p == pieces - 1
            ins += back[p][h if last else 0]
            specs += [pl.BlockSpec((half, width), local if last else here)] * slabs
        mine, give = pl.pallas_call(
            functools.partial(rows_inverse, first, slabs),
            grid_spec=pltpu.PrefetchScalarGridSpec(
                num_scalar_prefetch=1,
                grid=(2,),
                in_specs=[
                    pl.BlockSpec((2, half, cols), lambda i, c, at=at: (0, at + (i + c[0]) % 2, 0)),
                    whole_of(w_i),
                    whole_of(tw),
                ]
                + specs,
                out_specs=[pl.BlockSpec((half, cols), kept)] * 2,
                scratch_shapes=scratch(half),
            ),
            out_shape=[shape(half, cols)] * 2,
            compiler_params=params(),
            cost_estimate=cost(n * cols),
        )(core, anomalies, w_i, tw, *ins)
        chip = mine + swap(give, 1)
        for step in range(1, groups.bit_length() - 1):
            chip = chip + swap(chip, 2**step)
        other = swap(chip, 1)
        prior = [] if product is None else [product]
        product = pl.pallas_call(
            place,
            grid_spec=pltpu.PrefetchScalarGridSpec(
                num_scalar_prefetch=1,
                grid=(2,),
                in_specs=[pl.BlockSpec((half, cols), kept)] * 2 + [anywhere] * len(prior),
                out_specs=pl.BlockSpec((half, cols), here),
            ),
            out_shape=shape(rows, cols),
            input_output_aliases={3: 0} if prior else {},
            compiler_params=params(),
            cost_estimate=cost(n),
        )(core, chip, other, *prior)
    return product


def solution(mesh):
    placed = (P("mem", "slab", None), P("slab", None), P(None, "slab"))
    return jax.shard_map(
        functools.partial(per_device, mesh.shape["slab"], mesh.shape["mem"]),
        mesh=mesh,
        in_specs=placed,
        out_specs=P("slab", None),
        check_vma=False,
    )
```
